128 devices in a mesh: lat: 16 (over z, x), lon: 4 (over y), lev: 2 (over core).
Axes of the slice: x: 4, y: 4, z: 4, core: 2. Of those that a mesh axis runs over, the one named last changes fastest.
Arguments:
- pressure: float32 [64, 256, 128, 128], P('lat', 'lon', 'lev'), may hold values from 0.2 to 1.8
- earlier: float32 [64, 256, 128, 128], P('lat', 'lon', 'lev'), may hold values from 0.2 to 1.8
- speed_square: float32 [64, 256, 128, 128], P('lat', 'lon', 'lev'), may hold values from 0.05 to 0.3
Outputs:
- pressure_end: float32 [64, 256, 128, 128], P('lat', 'lon', 'lev')
The draws below stay inside these ranges and needn't reach their ends.
All inputs are finite; a program needn't handle non-finite values.
Results may differ from the reference program's by a relative error of at most 0.00002.
Values sent between devices are 32-bit elements.
A program may use at most 320 MiB of HBM per device.

```python
import jax
import jax.numpy as jnp
from jax import lax

GRID_Y = 64
GRID_X = 256
GRID_Z = 128
LEVELS = 128
STEPS = 4


def block_levels(stream_key, extent, cuts, least, high):
    def one(dim, shards_of):
        steps = jax.random.uniform(jax.random.fold_in(jax.random.fold_in(stream_key, 6), dim), (shards_of,), jnp.float32, least / len(cuts), high / len(cuts))
        return jnp.repeat(jnp.exp(steps), extent[dim] // shards_of).reshape((-1,) + (1,) * (len(extent) - dim - 1))

    factor_of = one(*cuts[0])
    for cut in cuts[1:]:
        factor_of = factor_of * one(*cut)
    return factor_of


def setup_inputs(seed: int = 0) -> dict:
    splits = jax.random.split(jax.random.key(seed), 4)
    return {
        "pressure": jnp.clip(0.2 + 1.5999999 * jax.random.uniform(splits[0], (GRID_Y, GRID_X, GRID_Z, LEVELS), jnp.float32) ** block_levels(splits[0], (GRID_Y, GRID_X, GRID_Z, LEVELS), ((0, 16), (1, 4), (2, 2)), -0.2, 0.2), 0.2, 1.8),
        "earlier": jnp.clip(0.2 + 1.5999999 * jax.random.uniform(splits[1], (GRID_Y, GRID_X, GRID_Z, LEVELS), jnp.float32) ** block_levels(splits[1], (GRID_Y, GRID_X, GRID_Z, LEVELS), ((0, 16), (1, 4), (2, 2)), -0.2, 0.2), 0.2, 1.8),
        "speed_square": jnp.clip(0.05 + 0.25 * jax.random.uniform(splits[2], (GRID_Y, GRID_X, GRID_Z, LEVELS), jnp.float32) ** block_levels(splits[2], (GRID_Y, GRID_X, GRID_Z, LEVELS), ((0, 16), (1, 4), (2, 2)), -0.2, 0.2), 0.05, 0.3),
    }


def inner_cells(values, dims):
    for dim in dims:
        values = lax.slice_in_dim(values, 1, values.shape[dim] - 1, axis=dim)
    return values


def side_cells(values, dim, start, dims):
    others = [other for other in dims if other != dim]
    values = inner_cells(values, others)
    return lax.slice_in_dim(values, start, start + values.shape[dim] - 2, axis=dim)


def advance(padded, before, speed_square):
    middle = inner_cells(padded, (0, 1, 2))
    lower = [side_cells(padded, dim, 0, (0, 1, 2)) for dim in (0, 1, 2)]
    upper = [side_cells(padded, dim, 2, (0, 1, 2)) for dim in (0, 1, 2)]
    spread = lower[0] + upper[0] + lower[1] + upper[1] + lower[2] + upper[2] - 6.0 * middle
    return 2.0 * middle - before + speed_square * spread


def reference(pressure, earlier, speed_square):
    for step in range(STEPS):
        later = advance(jnp.pad(pressure, ((1, 1), (1, 1), (1, 1), (0, 0)), mode="constant"), earlier, speed_square)
        earlier, pressure = pressure, later
    return pressure
```

```python
import jax
import jax.numpy as jnp
from jax import lax
from jax.experimental import pallas as pl
from jax.experimental.pallas import tpu as pltpu
from jax.sharding import PartitionSpec as P

STEPS = 4
CHUNKS = 8
MESH = pl.DeviceIdType.MESH


def kernel(
    p_in, e_in, c_in, out, even, odd, c, z_out, z_in,
    load_sem, y_send, y_recv, x_send, x_recv, z_send, z_recv,
):
    planes, rows, depth, levels = p_in.shape
    size = rows // CHUNKS
    lat, lon, lev = (lax.axis_index(name) for name in ("lat", "lon", "lev"))
    field = (even, odd)
    y_has = (lat > 0, lat < lax.axis_size("lat") - 1)
    x_has = (lon > 0, lon < lax.axis_size("lon") - 1)
    y_to = ({"lat": lat - 1}, {"lat": lat + 1})
    x_to = ({"lon": lon - 1}, {"lon": lon + 1})
    z_to = {"lev": 1 - lev}

    def y_rows(chunk, pad):
        return pl.ds(pad + chunk * size, size)

    def y_start(t, side, chunk):
        if t == 0:
            source = p_in.at[(0, planes - 1)[side], y_rows(chunk, 0)]
        else:
            source = field[t % 2].at[(1, planes)[side], y_rows(chunk, 1)]
        return pltpu.make_async_remote_copy(
            src_ref=source,
            dst_ref=field[t % 2].at[(planes + 1, 0)[side], y_rows(chunk, 1)],
            send_sem=y_send.at[t, side, chunk],
            recv_sem=y_recv.at[t, 1 - side, chunk],
            device_id=y_to[side],
            device_id_type=MESH,
        )

    def y_arrival(t, side, chunk):
        halo = field[t % 2].at[(0, planes + 1)[side], y_rows(chunk, 1)]
        return pltpu.make_async_remote_copy(
            src_ref=halo,
            dst_ref=halo,
            send_sem=y_send.at[t, side, chunk],
            recv_sem=y_recv.at[t, side, chunk],
            device_id=y_to[side],
            device_id_type=MESH,
        )

    def x_start(t, side):
        if t == 0:
            source = p_in.at[:, (0, rows - 1)[side]]
        else:
            source = field[t % 2].at[pl.ds(1, planes), (1, rows)[side]]
        return pltpu.make_async_remote_copy(
            src_ref=source,
            dst_ref=field[t % 2].at[pl.ds(1, planes), (rows + 1, 0)[side]],
            send_sem=x_send.at[t, side],
            recv_sem=x_recv.at[t, 1 - side],
            device_id=x_to[side],
            device_id_type=MESH,
        )

    def x_arrival(t, side):
        halo = field[t % 2].at[pl.ds(1, planes), (0, rows + 1)[side]]
        return pltpu.make_async_remote_copy(
            src_ref=halo,
            dst_ref=halo,
            send_sem=x_send.at[t, side],
            recv_sem=x_recv.at[t, side],
            device_id=x_to[side],
            device_id_type=MESH,
        )

    def z_copy(t):
        return pltpu.make_async_remote_copy(
            src_ref=z_out.at[t],
            dst_ref=z_in.at[t],
            send_sem=z_send.at[t],
            recv_sem=z_recv.at[t],
            device_id=z_to,
            device_id_type=MESH,
        )

    def on_sides(has, action):
        for side in (0, 1):
            pl.when(has[side])(lambda side=side: action(side))

    inner = (pl.ds(1, planes), pl.ds(1, rows))
    loads = [
        pltpu.make_async_copy(p_in, even.at[inner], load_sem.at[0]),
        pltpu.make_async_copy(e_in, odd.at[inner], load_sem.at[1]),
        pltpu.make_async_copy(c_in, c, load_sem.at[2]),
    ]
    for load in loads:
        load.start()
    barrier = pltpu.get_barrier_semaphore()

    def greet(device):
        pl.semaphore_signal(barrier, inc=1, device_id=device, device_id_type=MESH)

    greet(z_to)
    on_sides(y_has, lambda side: greet(y_to[side]))
    on_sides(x_has, lambda side: greet(x_to[side]))
    peers = 1 + sum(jnp.where(has, 1, 0) for has in y_has + x_has)
    pl.semaphore_wait(barrier, peers)

    def first_sends(chunk, carry):
        on_sides(y_has, lambda side: y_start(0, side, chunk).start())
        return carry

    lax.fori_loop(0, CHUNKS, first_sends, 0)
    on_sides(x_has, lambda side: x_start(0, side).start())

    nothing = jnp.zeros((depth, levels), jnp.float32)

    def clear_plane(side):
        @pl.when(jnp.logical_not(y_has[side]))
        def _():
            def one(row, carry):
                for ref in field:
                    ref[(0, planes + 1)[side], row + 1] = nothing
                return carry

            lax.fori_loop(0, rows, one, 0)

    def clear_row(side):
        @pl.when(jnp.logical_not(x_has[side]))
        def _():
            for ref in field:
                for plane in range(planes):
                    ref[plane + 1, (0, rows + 1)[side]] = nothing

    for side in (0, 1):
        clear_plane(side)
        clear_row(side)

    below, above = (lev == 1), (lev == 0)
    place = lax.broadcasted_iota(jnp.int32, (depth, levels), 0)

    def keep_face(t, plane, row, values):
        face = jnp.where(above, values[depth - 1 :], values[:1])
        z_out[t, plane, pl.ds(row, 1)] = face

    def advance(t, plane, row):
        now, other = field[t % 2], field[1 - t % 2]
        middle = now[plane + 1, row + 1]
        beside = z_in[t, plane, pl.ds(row, 1)]
        lower = jnp.where(place == 0, jnp.where(below, beside, 0.0), pltpu.roll(middle, 1, 0))
        upper = jnp.where(
            place == depth - 1, jnp.where(above, beside, 0.0), pltpu.roll(middle, depth - 1, 0)
        )
        total = now[plane, row + 1] + now[plane + 2, row + 1]
        total = total + now[plane + 1, row] + now[plane + 1, row + 2] + lower + upper
        spread = total - 6.0 * middle
        later = 2.0 * middle - other[plane + 1, row + 1] + c[plane, row] * spread
        if t < STEPS - 1:
            other[plane + 1, row + 1] = later
            keep_face(t + 1, plane, row, later)
        else:
            out[plane, row] = later

    for load in loads:
        load.wait()

    def first_face(row, carry):
        for plane in range(planes):
            keep_face(0, plane, row, even[plane + 1, row + 1])
        return carry

    lax.fori_loop(0, rows, first_face, 0)
    z_copy(0).start()

    for t in range(STEPS):
        if t > 0:
            on_sides(x_has, lambda side: x_start(t - 1, side).wait_send())
        on_sides(x_has, lambda side: x_arrival(t, side).wait_recv())
        z_copy(t).wait_recv()

        def inside(row, carry):
            for plane in range(1, planes - 1):
                advance(t, plane, row)
            return carry

        lax.fori_loop(0, rows, inside, 0)

        def outside(chunk, carry):
            if t > 0:
                on_sides(y_has, lambda side: y_start(t - 1, side, chunk).wait_send())
            on_sides(y_has, lambda side: y_arrival(t, side, chunk).wait_recv())

            def one(row, carry):
                for plane in (0, planes - 1):
                    advance(t, plane, chunk * size + row)
                return carry

            lax.fori_loop(0, size, one, 0)
            if t < STEPS - 1:
                on_sides(y_has, lambda side: y_start(t + 1, side, chunk).start())
            return carry

        lax.fori_loop(0, CHUNKS, outside, 0)
        if t < STEPS - 1:
            on_sides(x_has, lambda side: x_start(t + 1, side).start())
            z_copy(t + 1).start()

    last = STEPS - 1

    def last_sends(chunk, carry):
        on_sides(y_has, lambda side: y_start(last, side, chunk).wait_send())
        return carry

    lax.fori_loop(0, CHUNKS, last_sends, 0)
    on_sides(x_has, lambda side: x_start(last, side).wait_send())
    for t in range(STEPS):
        z_copy(t).wait_send()


def shards(pressure, earlier, speed_square):
    planes, rows, depth, levels = pressure.shape
    padded = (planes + 2, rows + 2, depth, levels)
    return pl.pallas_call(
        kernel,
        out_shape=pltpu.VMEM(pressure.shape, jnp.float32),
        in_specs=[pl.BlockSpec(memory_space=pltpu.HBM)] * 3,
        out_specs=pl.BlockSpec(memory_space=pltpu.VMEM),
        scratch_shapes=[
            pltpu.VMEM(padded, jnp.float32),
            pltpu.VMEM(padded, jnp.float32),
            pltpu.VMEM(pressure.shape, jnp.float32),
            pltpu.VMEM((STEPS, planes, rows, levels), jnp.float32),
            pltpu.VMEM((STEPS, planes, rows, levels), jnp.float32),
            pltpu.SemaphoreType.DMA((3,)),
            pltpu.SemaphoreType.DMA((STEPS, 2, CHUNKS)),
            pltpu.SemaphoreType.DMA((STEPS, 2, CHUNKS)),
            pltpu.SemaphoreType.DMA((STEPS, 2)),
            pltpu.SemaphoreType.DMA((STEPS, 2)),
            pltpu.SemaphoreType.DMA((STEPS,)),
            pltpu.SemaphoreType.DMA((STEPS,)),
        ],
        compiler_params=pltpu.CompilerParams(
            collective_id=0, has_side_effects=True, vmem_limit_bytes=48 * 2**20
        ),
    )(pressure, earlier, speed_square)


def solution(mesh):
    spec = P("lat", "lon", "lev", None)
    return jax.shard_map(
        shards, mesh=mesh, in_specs=(spec,) * 3, out_specs=spec, check_vma=False
    )
```

```python
import jax
import jax.numpy as jnp
from jax import lax
from jax.experimental import pallas as pl
from jax.experimental.pallas import tpu as pltpu
from jax.sharding import PartitionSpec as P

STEPS = 4
CHUNKS = 8
MESH = pl.DeviceIdType.MESH


def kernel(
    p_in, e_in, c_in, out, even, odd, c, z_out, z_in,
    load_sem, y_send, y_recv, x_send, x_recv, z_send, z_recv,
):
    planes, rows, depth, levels = p_in.shape
    size = rows // CHUNKS
    lat, lon, lev = (lax.axis_index(name) for name in ("lat", "lon", "lev"))
    field = (even, odd)
    y_has = (lat > 0, lat < lax.axis_size("lat") - 1)
    x_has = (lon > 0, lon < lax.axis_size("lon") - 1)
    y_to = ({"lat": lat - 1}, {"lat": lat + 1})
    x_to = ({"lon": lon - 1}, {"lon": lon + 1})
    z_to = {"lev": 1 - lev}

    def y_rows(chunk):
        return pl.ds(1 + chunk * size, size)

    def y_start(t, side, chunk):
        return pltpu.make_async_remote_copy(
            src_ref=field[t % 2].at[(1, planes)[side], y_rows(chunk)],
            dst_ref=field[t % 2].at[(planes + 1, 0)[side], y_rows(chunk)],
            send_sem=y_send.at[t, side, chunk],
            recv_sem=y_recv.at[t, 1 - side, chunk],
            device_id=y_to[side],
            device_id_type=MESH,
        )

    def y_arrival(t, side, chunk):
        halo = field[t % 2].at[(0, planes + 1)[side], y_rows(chunk)]
        return pltpu.make_async_remote_copy(
            src_ref=halo,
            dst_ref=halo,
            send_sem=y_send.at[t, side, chunk],
            recv_sem=y_recv.at[t, side, chunk],
            device_id=y_to[side],
            device_id_type=MESH,
        )

    def x_start(t, side):
        if t == 0:
            source = p_in.at[:, (0, rows - 1)[side]]
        else:
            source = field[t % 2].at[pl.ds(1, planes), (1, rows)[side]]
        return pltpu.make_async_remote_copy(
            src_ref=source,
            dst_ref=field[t % 2].at[pl.ds(1, planes), (rows + 1, 0)[side]],
            send_sem=x_send.at[t, side],
            recv_sem=x_recv.at[t, 1 - side],
            device_id=x_to[side],
            device_id_type=MESH,
        )

    def x_arrival(t, side):
        halo = field[t % 2].at[pl.ds(1, planes), (0, rows + 1)[side]]
        return pltpu.make_async_remote_copy(
            src_ref=halo,
            dst_ref=halo,
            send_sem=x_send.at[t, side],
            recv_sem=x_recv.at[t, side],
            device_id=x_to[side],
            device_id_type=MESH,
        )

    def z_copy(t):
        return pltpu.make_async_remote_copy(
            src_ref=z_out.at[t],
            dst_ref=z_in.at[t],
            send_sem=z_send.at[t],
            recv_sem=z_recv.at[t],
            device_id=z_to,
            device_id_type=MESH,
        )

    def on_sides(has, action):
        for side in (0, 1):
            pl.when(has[side])(lambda side=side: action(side))

    barrier = pltpu.get_barrier_semaphore()

    def greet(device):
        pl.semaphore_signal(barrier, inc=1, device_id=device, device_id_type=MESH)

    on_sides(y_has, lambda side: greet(y_to[side]))
    on_sides(x_has, lambda side: greet(x_to[side]))
    greet(z_to)

    def load_pressure(number, first, count, start, length):
        return pltpu.make_async_copy(
            p_in.at[pl.ds(first, count), pl.ds(start, length)],
            even.at[pl.ds(first + 1, count), pl.ds(start + 1, length)],
            load_sem.at[number],
        )

    heads = [load_pressure(side, (0, planes - 1)[side], 1, 0, size) for side in (0, 1)]
    tails = [
        load_pressure(2 + side, (0, planes - 1)[side], 1, size, rows - size) for side in (0, 1)
    ]
    loads = [
        load_pressure(4, 1, planes - 2, 0, rows),
        pltpu.make_async_copy(
            e_in, odd.at[pl.ds(1, planes), pl.ds(1, rows)], load_sem.at[5]
        ),
        pltpu.make_async_copy(c_in, c, load_sem.at[6]),
    ]
    for load in heads + tails + loads:
        load.start()
    peers = 1 + sum(jnp.where(has, 1, 0) for has in y_has + x_has)
    pl.semaphore_wait(barrier, peers)
    for load in heads:
        load.wait()
    on_sides(y_has, lambda side: y_start(0, side, 0).start())
    for load in tails:
        load.wait()

    def first_sends(chunk, carry):
        on_sides(y_has, lambda side: y_start(0, side, chunk).start())
        return carry

    lax.fori_loop(1, CHUNKS, first_sends, 0)
    on_sides(x_has, lambda side: x_start(0, side).start())

    nothing = jnp.zeros((depth, levels), jnp.float32)

    def clear_plane(side):
        @pl.when(jnp.logical_not(y_has[side]))
        def _():
            def one(row, carry):
                for ref in field:
                    ref[(0, planes + 1)[side], row + 1] = nothing
                return carry

            lax.fori_loop(0, rows, one, 0)

    def clear_row(side):
        @pl.when(jnp.logical_not(x_has[side]))
        def _():
            for ref in field:
                for plane in range(planes):
                    ref[plane + 1, (0, rows + 1)[side]] = nothing

    for side in (0, 1):
        clear_plane(side)
        clear_row(side)

    below, above = (lev == 1), (lev == 0)
    place = lax.broadcasted_iota(jnp.int32, (depth, levels), 0)

    def keep_face(t, plane, row, values):
        face = jnp.where(above, values[depth - 1 :], values[:1])
        z_out[t, plane, pl.ds(row, 1)] = face

    def advance(t, plane, row):
        now, other = field[t % 2], field[1 - t % 2]
        last = t == STEPS - 1
        middle = now[plane + 1, row + 1]
        beside = z_in[t, plane, pl.ds(row, 1)]
        lower = jnp.where(place == 0, jnp.where(below, beside, 0.0), pltpu.roll(middle, 1, 0))
        upper = jnp.where(
            place == depth - 1, jnp.where(above, beside, 0.0), pltpu.roll(middle, depth - 1, 0)
        )
        total = now[plane + 1, row] + now[plane + 1, row + 2] + lower + upper
        if not (last and plane == 0):
            total = total + now[plane, row + 1]
        if not (last and plane == planes - 1):
            total = total + now[plane + 2, row + 1]
        spread = total - 6.0 * middle
        later = 2.0 * middle - other[plane + 1, row + 1] + c[plane, row] * spread
        if last:
            out[plane, row] = later
        else:
            other[plane + 1, row + 1] = later
            keep_face(t + 1, plane, row, later)

    for load in loads:
        load.wait()

    def first_face(row, carry):
        for plane in range(planes):
            keep_face(0, plane, row, even[plane + 1, row + 1])
        return carry

    lax.fori_loop(0, rows, first_face, 0)
    z_copy(0).start()

    for t in range(STEPS):
        last = t == STEPS - 1
        if t > 0:
            on_sides(x_has, lambda side: x_start(t - 1, side).wait_send())
        on_sides(x_has, lambda side: x_arrival(t, side).wait_recv())
        z_copy(t).wait_recv()

        def inside(row, carry):
            for plane in range(planes) if last else range(1, planes - 1):
                advance(t, plane, row)
            return carry

        lax.fori_loop(0, rows, inside, 0)
        if last:
            break

        def outside(chunk, carry):
            if t > 0:
                on_sides(y_has, lambda side: y_start(t - 1, side, chunk).wait_send())
            on_sides(y_has, lambda side: y_arrival(t, side, chunk).wait_recv())

            def one(row, carry):
                for plane in (0, planes - 1):
                    advance(t, plane, chunk * size + row)
                return carry

            lax.fori_loop(0, size, one, 0)
            on_sides(y_has, lambda side: y_start(t + 1, side, chunk).start())
            return carry

        lax.fori_loop(0, CHUNKS, outside, 0)
        on_sides(x_has, lambda side: x_start(t + 1, side).start())
        z_copy(t + 1).start()

    t = STEPS - 1
    on_sides(x_has, lambda side: x_start(t, side).wait_send())
    for step in range(STEPS):
        z_copy(step).wait_send()

    def closing(chunk, carry):
        on_sides(y_has, lambda side: y_start(t - 1, side, chunk).wait_send())

        def add(side):
            y_arrival(t, side, chunk).wait_recv()
            plane = (0, planes - 1)[side]
            here = pl.ds(chunk * size, size)
            halo = field[t % 2][(0, planes + 1)[side], y_rows(chunk)]
            out[plane, here] = out[plane, here] + c[plane, here] * halo

        on_sides(y_has, add)
        on_sides(y_has, lambda side: y_start(t, side, chunk).wait_send())
        return carry

    lax.fori_loop(0, CHUNKS, closing, 0)


def shards(pressure, earlier, speed_square):
    planes, rows, depth, levels = pressure.shape
    padded = (planes + 2, rows + 2, depth, levels)
    return pl.pallas_call(
        kernel,
        out_shape=pltpu.VMEM(pressure.shape, jnp.float32),
        in_specs=[pl.BlockSpec(memory_space=pltpu.HBM)] * 3,
        out_specs=pl.BlockSpec(memory_space=pltpu.VMEM),
        scratch_shapes=[
            pltpu.VMEM(padded, jnp.float32),
            pltpu.VMEM(padded, jnp.float32),
            pltpu.VMEM(pressure.shape, jnp.float32),
            pltpu.VMEM((STEPS, planes, rows, levels), jnp.float32),
            pltpu.VMEM((STEPS, planes, rows, levels), jnp.float32),
            pltpu.SemaphoreType.DMA((7,)),
            pltpu.SemaphoreType.DMA((STEPS, 2, CHUNKS)),
            pltpu.SemaphoreType.DMA((STEPS, 2, CHUNKS)),
            pltpu.SemaphoreType.DMA((STEPS, 2)),
            pltpu.SemaphoreType.DMA((STEPS, 2)),
            pltpu.SemaphoreType.DMA((STEPS,)),
            pltpu.SemaphoreType.DMA((STEPS,)),
        ],
        compiler_params=pltpu.CompilerParams(
            collective_id=0, has_side_effects=True, vmem_limit_bytes=48 * 2**20
        ),
    )(pressure, earlier, speed_square)


def solution(mesh):
    spec = P("lat", "lon", "lev", None)
    return jax.shard_map(
        shards, mesh=mesh, in_specs=(spec,) * 3, out_specs=spec, check_vma=False
    )
```

```python
import jax
import jax.numpy as jnp
from jax import lax
from jax.experimental import pallas as pl
from jax.experimental.pallas import tpu as pltpu
from jax.sharding import PartitionSpec as P

STEPS = 4
CUTS = (0, 28, 56, 64)
CHUNKS = len(CUTS) - 1
RING = 4
RELIEF = 2
MESH = pl.DeviceIdType.MESH


def kernel(
    p_in, e_in, c_in, out, even, odd, c, z_out, z_in,
    passed, load_sem, y_send, y_recv, x_send, x_recv, z_send, z_recv, hop_sem,
):
    planes, rows, depth, levels = p_in.shape
    lat, lon, lev = (lax.axis_index(name) for name in ("lat", "lon", "lev"))
    field = (even, odd)
    y_has = (lat > 0, lat < lax.axis_size("lat") - 1)
    x_has = (lon > 0, lon < lax.axis_size("lon") - 1)
    y_to = ({"lat": lat - 1}, {"lat": lat + 1})
    x_to = ({"lon": lon - 1}, {"lon": lon + 1})
    z_to = {"lev": 1 - lev}

    rings = lax.axis_size("lat") // RING
    detours = []
    for q in range(rings - 1):
        end, start = q * RING + RING - 1, q * RING + RING
        detours.append((1, end, end + RING, start, RELIEF * (q + 1)))
        detours.append((0, start, start - RING, end, RELIEF * (rings - 1 - q)))
    ring_place = lax.rem(lat, RING)
    at_start, at_end = (ring_place == 0), (ring_place == RING - 1)
    wraps = (at_start, at_end)

    def hop(side, relay, count):
        return pltpu.make_async_remote_copy(
            src_ref=field[0].at[(1, planes)[side], pl.ds(1 + rows - count, count)],
            dst_ref=passed.at[pl.ds(0, count)],
            send_sem=hop_sem.at[0],
            recv_sem=hop_sem.at[1],
            device_id={"lat": relay},
            device_id_type=MESH,
        )

    def forward(side, dest, count):
        return pltpu.make_async_remote_copy(
            src_ref=passed.at[pl.ds(0, count)],
            dst_ref=field[0].at[(planes + 1, 0)[side], pl.ds(1 + rows - count, count)],
            send_sem=hop_sem.at[2],
            recv_sem=hop_sem.at[3],
            device_id={"lat": dest},
            device_id_type=MESH,
        )

    def y_rows(chunk, less=0):
        return pl.ds(1 + CUTS[chunk], CUTS[chunk + 1] - CUTS[chunk] - less)

    def y_start(t, side, chunk, less=0):
        return pltpu.make_async_remote_copy(
            src_ref=field[t % 2].at[(1, planes)[side], y_rows(chunk, less)],
            dst_ref=field[t % 2].at[(planes + 1, 0)[side], y_rows(chunk, less)],
            send_sem=y_send.at[t, side, chunk],
            recv_sem=y_recv.at[t, 1 - side, chunk],
            device_id=y_to[side],
            device_id_type=MESH,
        )

    def y_arrival(t, side, chunk, less=0):
        halo = field[t % 2].at[(0, planes + 1)[side], y_rows(chunk, less)]
        return pltpu.make_async_remote_copy(
            src_ref=halo,
            dst_ref=halo,
            send_sem=y_send.at[t, side, chunk],
            recv_sem=y_recv.at[t, side, chunk],
            device_id=y_to[side],
            device_id_type=MESH,
        )

    def sending(t, chunk, action):
        detoured = t == 0 and chunk == CHUNKS - 1
        for side in (0, 1):
            direct = y_has[side]
            if detoured:
                direct = direct & jnp.logical_not(wraps[side])
            pl.when(direct)(lambda side=side: action(y_start(t, side, chunk)))
        for side, origin, relay, dest, count in detours if detoured else ():

            @pl.when(lat == origin)
            def _():
                action(y_start(t, side, chunk, count))
                action(hop(side, relay, count))

    def arriving(t, side, chunk):
        detoured = t == 0 and chunk == CHUNKS - 1
        direct = y_has[side]
        if detoured:
            direct = direct & jnp.logical_not(wraps[side])
        pl.when(direct)(lambda: y_arrival(t, side, chunk).wait_recv())
        for way, origin, relay, dest, count in detours if detoured else ():
            if way != side:

                @pl.when(lat == dest)
                def _():
                    y_arrival(t, side, chunk, count).wait_recv()
                    forward(way, dest, count).wait_recv()

    def x_start(t, side):
        if t == 0:
            source = p_in.at[:, (0, rows - 1)[side]]
        else:
            source = field[t % 2].at[pl.ds(1, planes), (1, rows)[side]]
        return pltpu.make_async_remote_copy(
            src_ref=source,
            dst_ref=field[t % 2].at[pl.ds(1, planes), (rows + 1, 0)[side]],
            send_sem=x_send.at[t, side],
            recv_sem=x_recv.at[t, 1 - side],
            device_id=x_to[side],
            device_id_type=MESH,
        )

    def x_arrival(t, side):
        halo = field[t % 2].at[pl.ds(1, planes), (0, rows + 1)[side]]
        return pltpu.make_async_remote_copy(
            src_ref=halo,
            dst_ref=halo,
            send_sem=x_send.at[t, side],
            recv_sem=x_recv.at[t, side],
            device_id=x_to[side],
            device_id_type=MESH,
        )

    def z_copy(t):
        return pltpu.make_async_remote_copy(
            src_ref=z_out.at[t],
            dst_ref=z_in.at[t],
            send_sem=z_send.at[t],
            recv_sem=z_recv.at[t],
            device_id=z_to,
            device_id_type=MESH,
        )

    def on_sides(has, action):
        for side in (0, 1):
            pl.when(has[side])(lambda side=side: action(side))

    barrier = pltpu.get_barrier_semaphore()

    def greet(device):
        pl.semaphore_signal(barrier, inc=1, device_id=device, device_id_type=MESH)

    on_sides(y_has, lambda side: greet(y_to[side]))
    on_sides(x_has, lambda side: greet(x_to[side]))
    greet(z_to)
    outer = at_start | at_end
    ring_has = (outer & (lat >= RING), outer & (lat < (rings - 1) * RING))
    if rings > 1:
        on_sides(ring_has, lambda side: greet({"lat": lat + (-RING, RING)[side]}))
        on_sides(wraps, lambda side: greet({"lat": lat + (RING - 1, 1 - RING)[side]}))

    def load_pressure(number, first, count, start, length):
        return pltpu.make_async_copy(
            p_in.at[pl.ds(first, count), pl.ds(start, length)],
            even.at[pl.ds(first + 1, count), pl.ds(start + 1, length)],
            load_sem.at[number],
        )

    ends = (0, planes - 1)
    heads = [load_pressure(side, ends[side], 1, 0, CUTS[1]) for side in (0, 1)]
    tails = [
        load_pressure(2 + side, ends[side], 1, CUTS[1], rows - CUTS[1]) for side in (0, 1)
    ]
    loads = [
        load_pressure(4, 1, planes - 2, 0, rows),
        pltpu.make_async_copy(
            e_in, odd.at[pl.ds(1, planes), pl.ds(1, rows)], load_sem.at[5]
        ),
        pltpu.make_async_copy(c_in, c, load_sem.at[6]),
    ]
    for load in heads + tails + loads:
        load.start()
    others = y_has + x_has + (ring_has + wraps if rings > 1 else ())
    peers = 1 + sum(jnp.where(has, 1, 0) for has in others)
    pl.semaphore_wait(barrier, peers)
    for load in heads:
        load.wait()
    sending(0, 0, lambda copy: copy.start())
    for load in tails:
        load.wait()

    for chunk in range(1, CHUNKS):
        sending(0, chunk, lambda copy: copy.start())
    on_sides(x_has, lambda side: x_start(0, side).start())

    nothing = jnp.zeros((depth, levels), jnp.float32)

    def clear_plane(side):
        @pl.when(jnp.logical_not(y_has[side]))
        def _():
            def one(row, carry):
                for ref in field:
                    ref[(0, planes + 1)[side], row + 1] = nothing
                return carry

            lax.fori_loop(0, rows, one, 0)

    def clear_row(side):
        @pl.when(jnp.logical_not(x_has[side]))
        def _():
            for ref in field:
                for plane in range(planes):
                    ref[plane + 1, (0, rows + 1)[side]] = nothing

    for side in (0, 1):
        clear_plane(side)
        clear_row(side)

    below, above = (lev == 1), (lev == 0)
    place = lax.broadcasted_iota(jnp.int32, (depth, levels), 0)

    def keep_face(t, plane, row, values):
        face = jnp.where(above, values[depth - 1 :], values[:1])
        z_out[t, plane, pl.ds(row, 1)] = face

    def advance(t, plane, row):
        now, other = field[t % 2], field[1 - t % 2]
        last = t == STEPS - 1
        middle = now[plane + 1, row + 1]
        beside = z_in[t, plane, pl.ds(row, 1)]
        lower = jnp.where(place == 0, jnp.where(below, beside, 0.0), pltpu.roll(middle, 1, 0))
        upper = jnp.where(
            place == depth - 1, jnp.where(above, beside, 0.0), pltpu.roll(middle, depth - 1, 0)
        )
        total = now[plane + 1, row] + now[plane + 1, row + 2] + lower + upper
        if not (last and plane == 0):
            total = total + now[plane, row + 1]
        if not (last and plane == planes - 1):
            total = total + now[plane + 2, row + 1]
        spread = total - 6.0 * middle
        later = 2.0 * middle - other[plane + 1, row + 1] + c[plane, row] * spread
        if last:
            out[plane, row] = later
        else:
            other[plane + 1, row + 1] = later
            keep_face(t + 1, plane, row, later)

    for load in loads:
        load.wait()

    def first_face(row, carry):
        for plane in range(planes):
            keep_face(0, plane, row, even[plane + 1, row + 1])
        return carry

    lax.fori_loop(0, rows, first_face, 0)
    z_copy(0).start()
    for way, origin, relay, dest, count in detours:

        @pl.when(lat == relay)
        def _():
            hop(way, relay, count).wait_recv()
            forward(way, dest, count).start()


    for t in range(STEPS):
        last = t == STEPS - 1
        if t > 0:
            on_sides(x_has, lambda side: x_start(t - 1, side).wait_send())
        on_sides(x_has, lambda side: x_arrival(t, side).wait_recv())
        z_copy(t).wait_recv()

        def inside(row, carry):
            for plane in range(planes) if last else range(1, planes - 1):
                advance(t, plane, row)
            return carry

        lax.fori_loop(0, rows, inside, 0)
        if last:
            break

        for chunk in range(CHUNKS):
            if t > 0:
                sending(t - 1, chunk, lambda copy: copy.wait_send())
            for side in (0, 1):
                arriving(t, side, chunk)

            def one(row, carry):
                for plane in (0, planes - 1):
                    advance(t, plane, row)
                return carry

            lax.fori_loop(CUTS[chunk], CUTS[chunk + 1], one, 0)
            sending(t + 1, chunk, lambda copy: copy.start())

        on_sides(x_has, lambda side: x_start(t + 1, side).start())
        z_copy(t + 1).start()

    for way, origin, relay, dest, count in detours:
        pl.when(lat == relay)(lambda: forward(way, dest, count).wait_send())
    t = STEPS - 1
    on_sides(x_has, lambda side: x_start(t, side).wait_send())
    for step in range(STEPS):
        z_copy(step).wait_send()

    for chunk in range(CHUNKS):
        sending(t - 1, chunk, lambda copy: copy.wait_send())

        def add(side):
            y_arrival(t, side, chunk).wait_recv()
            plane = (0, planes - 1)[side]

            def one(row, carry):
                halo = field[t % 2][(0, planes + 1)[side], row + 1]
                out[plane, row] = out[plane, row] + c[plane, row] * halo
                return carry

            lax.fori_loop(CUTS[chunk], CUTS[chunk + 1], one, 0, unroll=4)

        on_sides(y_has, add)
        sending(t, chunk, lambda copy: copy.wait_send())


def shards(pressure, earlier, speed_square):
    planes, rows, depth, levels = pressure.shape
    padded = (planes + 2, rows + 2, depth, levels)
    return pl.pallas_call(
        kernel,
        out_shape=pltpu.VMEM(pressure.shape, jnp.float32),
        in_specs=[pl.BlockSpec(memory_space=pltpu.HBM)] * 3,
        out_specs=pl.BlockSpec(memory_space=pltpu.VMEM),
        scratch_shapes=[
            pltpu.VMEM(padded, jnp.float32),
            pltpu.VMEM(padded, jnp.float32),
            pltpu.VMEM(pressure.shape, jnp.float32),
            pltpu.VMEM((STEPS, planes, rows, levels), jnp.float32),
            pltpu.VMEM((STEPS, planes, rows, levels), jnp.float32),
            pltpu.VMEM((CUTS[-1] - CUTS[-2],) + pressure.shape[2:], jnp.float32),
            pltpu.SemaphoreType.DMA((7,)),
            pltpu.SemaphoreType.DMA((STEPS, 2, CHUNKS)),
            pltpu.SemaphoreType.DMA((STEPS, 2, CHUNKS)),
            pltpu.SemaphoreType.DMA((STEPS, 2)),
            pltpu.SemaphoreType.DMA((STEPS, 2)),
            pltpu.SemaphoreType.DMA((STEPS,)),
            pltpu.SemaphoreType.DMA((STEPS,)),
            pltpu.SemaphoreType.DMA((4,)),
        ],
        compiler_params=pltpu.CompilerParams(
            collective_id=0, has_side_effects=True, vmem_limit_bytes=48 * 2**20
        ),
    )(pressure, earlier, speed_square)


def solution(mesh):
    spec = P("lat", "lon", "lev", None)
    return jax.shard_map(
        shards, mesh=mesh, in_specs=(spec,) * 3, out_specs=spec, check_vma=False
    )
```

```python
import jax
import jax.numpy as jnp
from jax import lax
from jax.experimental import pallas as pl
from jax.experimental.pallas import tpu as pltpu
from jax.sharding import PartitionSpec as P

STEPS = 4
CUTS = (0, 30, 60, 64)
CHUNKS = len(CUTS) - 1
RING = 4
RELIEF = 3
MESH = pl.DeviceIdType.MESH


def kernel(
    p_in, e_in, c_in, out, even, odd, c, z_out, z_in,
    passed, load_sem, y_send, y_recv, x_send, x_recv, z_send, z_recv, hop_sem,
):
    planes, rows, depth, levels = p_in.shape
    lat, lon, lev = (lax.axis_index(name) for name in ("lat", "lon", "lev"))
    field = (even, odd)
    y_has = (lat > 0, lat < lax.axis_size("lat") - 1)
    x_has = (lon > 0, lon < lax.axis_size("lon") - 1)
    y_to = ({"lat": lat - 1}, {"lat": lat + 1})
    x_to = ({"lon": lon - 1}, {"lon": lon + 1})
    z_to = {"lev": 1 - lev}

    rings = lax.axis_size("lat") // RING
    detours = []
    for q in range(rings - 1):
        end, start = q * RING + RING - 1, q * RING + RING
        detours.append((1, end, end + RING, start, RELIEF * (q + 1)))
        detours.append((0, start, start - RING, end, RELIEF * (rings - 1 - q)))
    ring_place = lax.rem(lat, RING)
    at_start, at_end = (ring_place == 0), (ring_place == RING - 1)
    wraps = (at_start, at_end)

    def hop(side, relay, count):
        return pltpu.make_async_remote_copy(
            src_ref=field[0].at[(1, planes)[side], pl.ds(1 + CUTS[2] - count, count)],
            dst_ref=passed.at[pl.ds(0, count)],
            send_sem=hop_sem.at[0],
            recv_sem=hop_sem.at[1],
            device_id={"lat": relay},
            device_id_type=MESH,
        )

    def forward(side, dest, count):
        return pltpu.make_async_remote_copy(
            src_ref=passed.at[pl.ds(0, count)],
            dst_ref=field[0].at[(planes + 1, 0)[side], pl.ds(1 + CUTS[2] - count, count)],
            send_sem=hop_sem.at[2],
            recv_sem=hop_sem.at[3],
            device_id={"lat": dest},
            device_id_type=MESH,
        )

    def y_rows(chunk, less=0):
        return pl.ds(1 + CUTS[chunk], CUTS[chunk + 1] - CUTS[chunk] - less)

    def y_start(t, side, chunk, less=0):
        return pltpu.make_async_remote_copy(
            src_ref=field[t % 2].at[(1, planes)[side], y_rows(chunk, less)],
            dst_ref=field[t % 2].at[(planes + 1, 0)[side], y_rows(chunk, less)],
            send_sem=y_send.at[t, side, chunk],
            recv_sem=y_recv.at[t, 1 - side, chunk],
            device_id=y_to[side],
            device_id_type=MESH,
        )

    def y_arrival(t, side, chunk, less=0):
        halo = field[t % 2].at[(0, planes + 1)[side], y_rows(chunk, less)]
        return pltpu.make_async_remote_copy(
            src_ref=halo,
            dst_ref=halo,
            send_sem=y_send.at[t, side, chunk],
            recv_sem=y_recv.at[t, side, chunk],
            device_id=y_to[side],
            device_id_type=MESH,
        )

    def sending(t, chunk, action):
        detoured = t == 0 and chunk == 1
        for side in (1, 0):
            direct = y_has[side]
            if detoured:
                direct = direct & jnp.logical_not(wraps[side])
            pl.when(direct)(lambda side=side: action(y_start(t, side, chunk)))
        for side, origin, relay, dest, count in detours if detoured else ():

            @pl.when(lat == origin)
            def _():
                action(y_start(t, side, chunk, count))
                action(hop(side, relay, count))

    def arriving(t, side, chunk):
        detoured = t == 0 and chunk == 1
        direct = y_has[side]
        if detoured:
            direct = direct & jnp.logical_not(wraps[side])
        pl.when(direct)(lambda: y_arrival(t, side, chunk).wait_recv())
        for way, origin, relay, dest, count in detours if detoured else ():
            if way != side:

                @pl.when(lat == dest)
                def _():
                    y_arrival(t, side, chunk, count).wait_recv()
                    forward(way, dest, count).wait_recv()

    def x_start(t, side):
        if t == 0:
            source = p_in.at[:, (0, rows - 1)[side]]
        else:
            source = field[t % 2].at[pl.ds(1, planes), (1, rows)[side]]
        return pltpu.make_async_remote_copy(
            src_ref=source,
            dst_ref=field[t % 2].at[pl.ds(1, planes), (rows + 1, 0)[side]],
            send_sem=x_send.at[t, side],
            recv_sem=x_recv.at[t, 1 - side],
            device_id=x_to[side],
            device_id_type=MESH,
        )

    def x_arrival(t, side):
        halo = field[t % 2].at[pl.ds(1, planes), (0, rows + 1)[side]]
        return pltpu.make_async_remote_copy(
            src_ref=halo,
            dst_ref=halo,
            send_sem=x_send.at[t, side],
            recv_sem=x_recv.at[t, side],
            device_id=x_to[side],
            device_id_type=MESH,
        )

    def z_copy(t):
        return pltpu.make_async_remote_copy(
            src_ref=z_out.at[t],
            dst_ref=z_in.at[t],
            send_sem=z_send.at[t],
            recv_sem=z_recv.at[t],
            device_id=z_to,
            device_id_type=MESH,
        )

    def on_sides(has, action):
        for side in (0, 1):
            pl.when(has[side])(lambda side=side: action(side))

    barrier = pltpu.get_barrier_semaphore()

    def greet(device):
        pl.semaphore_signal(barrier, inc=1, device_id=device, device_id_type=MESH)

    on_sides(y_has, lambda side: greet(y_to[side]))
    on_sides(x_has, lambda side: greet(x_to[side]))
    greet(z_to)
    outer = at_start | at_end
    ring_has = (outer & (lat >= RING), outer & (lat < (rings - 1) * RING))
    if rings > 1:
        on_sides(ring_has, lambda side: greet({"lat": lat + (-RING, RING)[side]}))
        on_sides(wraps, lambda side: greet({"lat": lat + (RING - 1, 1 - RING)[side]}))

    def load_pressure(number, first, count, start, length):
        return pltpu.make_async_copy(
            p_in.at[pl.ds(first, count), pl.ds(start, length)],
            even.at[pl.ds(first + 1, count), pl.ds(start + 1, length)],
            load_sem.at[number],
        )

    ends = (0, planes - 1)
    heads = [load_pressure(side, ends[side], 1, 0, CUTS[1]) for side in (0, 1)]
    tails = [
        load_pressure(2 + side, ends[side], 1, CUTS[1], rows - CUTS[1]) for side in (0, 1)
    ]
    loads = [
        load_pressure(4, 1, planes - 2, 0, rows),
        pltpu.make_async_copy(
            e_in, odd.at[pl.ds(1, planes), pl.ds(1, rows)], load_sem.at[5]
        ),
        pltpu.make_async_copy(c_in, c, load_sem.at[6]),
    ]
    for load in heads + tails + loads:
        load.start()
    others = y_has + x_has + (ring_has + wraps if rings > 1 else ())
    peers = 1 + sum(jnp.where(has, 1, 0) for has in others)
    pl.semaphore_wait(barrier, peers)
    for load in heads:
        load.wait()
    sending(0, 0, lambda copy: copy.start())
    for load in tails:
        load.wait()

    for chunk in range(1, CHUNKS):
        sending(0, chunk, lambda copy: copy.start())
    on_sides(x_has, lambda side: x_start(0, side).start())

    nothing = jnp.zeros((depth, levels), jnp.float32)

    def clear_plane(side):
        @pl.when(jnp.logical_not(y_has[side]))
        def _():
            def one(row, carry):
                for ref in field:
                    ref[(0, planes + 1)[side], row + 1] = nothing
                return carry

            lax.fori_loop(0, rows, one, 0)

    def clear_row(side):
        @pl.when(jnp.logical_not(x_has[side]))
        def _():
            for ref in field:
                for plane in range(planes):
                    ref[plane + 1, (0, rows + 1)[side]] = nothing

    for side in (0, 1):
        clear_plane(side)
        clear_row(side)

    below, above = (lev == 1), (lev == 0)
    place = lax.broadcasted_iota(jnp.int32, (depth, levels), 0)

    def keep_face(t, plane, row, values):
        face = jnp.where(above, values[depth - 1 :], values[:1])
        z_out[t, plane, pl.ds(row, 1)] = face

    def advance(t, plane, row):
        now, other = field[t % 2], field[1 - t % 2]
        last = t == STEPS - 1
        middle = now[plane + 1, row + 1]
        beside = z_in[t, plane, pl.ds(row, 1)]
        lower = jnp.where(place == 0, jnp.where(below, beside, 0.0), pltpu.roll(middle, 1, 0))
        upper = jnp.where(
            place == depth - 1, jnp.where(above, beside, 0.0), pltpu.roll(middle, depth - 1, 0)
        )
        total = now[plane + 1, row] + now[plane + 1, row + 2] + lower + upper
        if not (last and plane == 0):
            total = total + now[plane, row + 1]
        if not (last and plane == planes - 1):
            total = total + now[plane + 2, row + 1]
        spread = total - 6.0 * middle
        later = 2.0 * middle - other[plane + 1, row + 1] + c[plane, row] * spread
        if last:
            out[plane, row] = later
        else:
            other[plane + 1, row + 1] = later
            keep_face(t + 1, plane, row, later)

    for load in loads:
        load.wait()

    def first_face(row, carry):
        for plane in range(planes):
            keep_face(0, plane, row, even[plane + 1, row + 1])
        return carry

    lax.fori_loop(0, rows, first_face, 0)
    z_copy(0).start()
    for way, origin, relay, dest, count in detours:

        @pl.when(lat == relay)
        def _():
            hop(way, relay, count).wait_recv()
            forward(way, dest, count).start()


    for t in range(STEPS):
        last = t == STEPS - 1
        if t > 0:
            on_sides(x_has, lambda side: x_start(t - 1, side).wait_send())
        on_sides(x_has, lambda side: x_arrival(t, side).wait_recv())
        z_copy(t).wait_recv()

        def inside(row, carry):
            for plane in range(planes) if last else range(1, planes - 1):
                advance(t, plane, row)
            return carry

        lax.fori_loop(0, rows, inside, 0)
        if last:
            break

        for chunk in range(CHUNKS):
            if t > 0:
                sending(t - 1, chunk, lambda copy: copy.wait_send())
            for side in (0, 1):
                arriving(t, side, chunk)

            def one(row, carry):
                for plane in (0, planes - 1):
                    advance(t, plane, row)
                return carry

            lax.fori_loop(CUTS[chunk], CUTS[chunk + 1], one, 0)
            sending(t + 1, chunk, lambda copy: copy.start())

        on_sides(x_has, lambda side: x_start(t + 1, side).start())
        z_copy(t + 1).start()

    for way, origin, relay, dest, count in detours:
        pl.when(lat == relay)(lambda: forward(way, dest, count).wait_send())
    t = STEPS - 1
    on_sides(x_has, lambda side: x_start(t, side).wait_send())
    for step in range(STEPS):
        z_copy(step).wait_send()

    for chunk in range(CHUNKS):
        sending(t - 1, chunk, lambda copy: copy.wait_send())

        def add(side):
            y_arrival(t, side, chunk).wait_recv()
            plane = (0, planes - 1)[side]

            def one(row, carry):
                halo = field[t % 2][(0, planes + 1)[side], row + 1]
                out[plane, row] = out[plane, row] + c[plane, row] * halo
                return carry

            lax.fori_loop(CUTS[chunk], CUTS[chunk + 1], one, 0, unroll=4)

        on_sides(y_has, add)
        sending(t, chunk, lambda copy: copy.wait_send())


def shards(pressure, earlier, speed_square):
    planes, rows, depth, levels = pressure.shape
    padded = (planes + 2, rows + 2, depth, levels)
    return pl.pallas_call(
        kernel,
        out_shape=pltpu.VMEM(pressure.shape, jnp.float32),
        in_specs=[pl.BlockSpec(memory_space=pltpu.HBM)] * 3,
        out_specs=pl.BlockSpec(memory_space=pltpu.VMEM),
        scratch_shapes=[
            pltpu.VMEM(padded, jnp.float32),
            pltpu.VMEM(padded, jnp.float32),
            pltpu.VMEM(pressure.shape, jnp.float32),
            pltpu.VMEM((STEPS, planes, rows, levels), jnp.float32),
            pltpu.VMEM((STEPS, planes, rows, levels), jnp.float32),
            pltpu.VMEM((RING * RELIEF,) + pressure.shape[2:], jnp.float32),
            pltpu.SemaphoreType.DMA((7,)),
            pltpu.SemaphoreType.DMA((STEPS, 2, CHUNKS)),
            pltpu.SemaphoreType.DMA((STEPS, 2, CHUNKS)),
            pltpu.SemaphoreType.DMA((STEPS, 2)),
            pltpu.SemaphoreType.DMA((STEPS, 2)),
            pltpu.SemaphoreType.DMA((STEPS,)),
            pltpu.SemaphoreType.DMA((STEPS,)),
            pltpu.SemaphoreType.DMA((4,)),
        ],
        compiler_params=pltpu.CompilerParams(
            collective_id=0, has_side_effects=True, vmem_limit_bytes=48 * 2**20
        ),
    )(pressure, earlier, speed_square)


def solution(mesh):
    spec = P("lat", "lon", "lev", None)
    return jax.shard_map(
        shards, mesh=mesh, in_specs=(spec,) * 3, out_specs=spec, check_vma=False
    )
```

```python
import jax
import jax.numpy as jnp
from jax import lax
from jax.experimental import pallas as pl
from jax.experimental.pallas import tpu as pltpu
from jax.sharding import PartitionSpec as P

STEPS = 4
CUTS = (0, 32, 64)
LAST_CUTS = (0, 32, 60, 64)
CHUNKS = len(CUTS) - 1
LAST_CHUNKS = len(LAST_CUTS) - 1
RING = 4
RELIEF = 3
MESH = pl.DeviceIdType.MESH


def kernel(
    p_in, e_in, c_in, out, even, odd, c, z_out, z_in,
    passed, load_sem, y_send, y_recv, x_send, x_recv, z_send, z_recv, hop_sem,
):
    planes, rows, depth, levels = p_in.shape
    lat, lon, lev = (lax.axis_index(name) for name in ("lat", "lon", "lev"))
    field = (even, odd)
    y_has = (lat > 0, lat < lax.axis_size("lat") - 1)
    x_has = (lon > 0, lon < lax.axis_size("lon") - 1)
    y_to = ({"lat": lat - 1}, {"lat": lat + 1})
    x_to = ({"lon": lon - 1}, {"lon": lon + 1})
    z_to = {"lev": 1 - lev}

    rings = lax.axis_size("lat") // RING
    detours = []
    for q in range(rings - 1):
        end, start = q * RING + RING - 1, q * RING + RING
        detours.append((1, end, end + RING, start, RELIEF * (q + 1)))
        detours.append((0, start, start - RING, end, RELIEF * (rings - 1 - q)))
    ring_place = lax.rem(lat, RING)
    at_start, at_end = (ring_place == 0), (ring_place == RING - 1)
    wraps = (at_start, at_end)

    def hop(side, relay, count):
        return pltpu.make_async_remote_copy(
            src_ref=field[0].at[(1, planes)[side], pl.ds(1 + CUTS[2] - count, count)],
            dst_ref=passed.at[pl.ds(0, count)],
            send_sem=hop_sem.at[0],
            recv_sem=hop_sem.at[1],
            device_id={"lat": relay},
            device_id_type=MESH,
        )

    def forward(side, dest, count):
        return pltpu.make_async_remote_copy(
            src_ref=passed.at[pl.ds(0, count)],
            dst_ref=field[0].at[(planes + 1, 0)[side], pl.ds(1 + CUTS[2] - count, count)],
            send_sem=hop_sem.at[2],
            recv_sem=hop_sem.at[3],
            device_id={"lat": dest},
            device_id_type=MESH,
        )

    def y_rows(t, chunk, less=0):
        cuts = LAST_CUTS if t == STEPS - 1 else CUTS
        return pl.ds(1 + cuts[chunk], cuts[chunk + 1] - cuts[chunk] - less)

    def y_start(t, side, chunk, less=0):
        return pltpu.make_async_remote_copy(
            src_ref=field[t % 2].at[(1, planes)[side], y_rows(t, chunk, less)],
            dst_ref=field[t % 2].at[(planes + 1, 0)[side], y_rows(t, chunk, less)],
            send_sem=y_send.at[t, side, chunk],
            recv_sem=y_recv.at[t, 1 - side, chunk],
            device_id=y_to[side],
            device_id_type=MESH,
        )

    def y_arrival(t, side, chunk, less=0):
        halo = field[t % 2].at[(0, planes + 1)[side], y_rows(t, chunk, less)]
        return pltpu.make_async_remote_copy(
            src_ref=halo,
            dst_ref=halo,
            send_sem=y_send.at[t, side, chunk],
            recv_sem=y_recv.at[t, side, chunk],
            device_id=y_to[side],
            device_id_type=MESH,
        )

    def sending(t, chunk, action):
        detoured = t == 0 and chunk == 1
        for side in (1, 0):
            direct = y_has[side]
            if detoured:
                direct = direct & jnp.logical_not(wraps[side])
            pl.when(direct)(lambda side=side: action(y_start(t, side, chunk)))
        for side, origin, relay, dest, count in detours if detoured else ():

            @pl.when(lat == origin)
            def _():
                action(y_start(t, side, chunk, count))
                action(hop(side, relay, count))

    def arriving(t, side, chunk):
        detoured = t == 0 and chunk == 1
        direct = y_has[side]
        if detoured:
            direct = direct & jnp.logical_not(wraps[side])
        pl.when(direct)(lambda: y_arrival(t, side, chunk).wait_recv())
        for way, origin, relay, dest, count in detours if detoured else ():
            if way != side:

                @pl.when(lat == dest)
                def _():
                    y_arrival(t, side, chunk, count).wait_recv()
                    forward(way, dest, count).wait_recv()

    def x_start(t, side):
        if t == 0:
            source = p_in.at[:, (0, rows - 1)[side]]
        else:
            source = field[t % 2].at[pl.ds(1, planes), (1, rows)[side]]
        return pltpu.make_async_remote_copy(
            src_ref=source,
            dst_ref=field[t % 2].at[pl.ds(1, planes), (rows + 1, 0)[side]],
            send_sem=x_send.at[t, side],
            recv_sem=x_recv.at[t, 1 - side],
            device_id=x_to[side],
            device_id_type=MESH,
        )

    def x_arrival(t, side):
        halo = field[t % 2].at[pl.ds(1, planes), (0, rows + 1)[side]]
        return pltpu.make_async_remote_copy(
            src_ref=halo,
            dst_ref=halo,
            send_sem=x_send.at[t, side],
            recv_sem=x_recv.at[t, side],
            device_id=x_to[side],
            device_id_type=MESH,
        )

    def z_copy(t):
        return pltpu.make_async_remote_copy(
            src_ref=z_out.at[t],
            dst_ref=z_in.at[t],
            send_sem=z_send.at[t],
            recv_sem=z_recv.at[t],
            device_id=z_to,
            device_id_type=MESH,
        )

    def on_sides(has, action):
        for side in (0, 1):
            pl.when(has[side])(lambda side=side: action(side))

    barrier = pltpu.get_barrier_semaphore()

    def greet(device):
        pl.semaphore_signal(barrier, inc=1, device_id=device, device_id_type=MESH)

    on_sides(y_has, lambda side: greet(y_to[side]))
    on_sides(x_has, lambda side: greet(x_to[side]))
    greet(z_to)
    outer = at_start | at_end
    ring_has = (outer & (lat >= RING), outer & (lat < (rings - 1) * RING))
    if rings > 1:
        on_sides(ring_has, lambda side: greet({"lat": lat + (-RING, RING)[side]}))
        on_sides(wraps, lambda side: greet({"lat": lat + (RING - 1, 1 - RING)[side]}))

    def load_pressure(number, first, count, start, length):
        return pltpu.make_async_copy(
            p_in.at[pl.ds(first, count), pl.ds(start, length)],
            even.at[pl.ds(first + 1, count), pl.ds(start + 1, length)],
            load_sem.at[number],
        )

    ends = (0, planes - 1)
    heads = [load_pressure(side, ends[side], 1, 0, CUTS[1]) for side in (0, 1)]
    tails = [
        load_pressure(2 + side, ends[side], 1, CUTS[1], rows - CUTS[1]) for side in (0, 1)
    ]
    loads = [
        load_pressure(4, 1, planes - 2, 0, rows),
        pltpu.make_async_copy(
            e_in, odd.at[pl.ds(1, planes), pl.ds(1, rows)], load_sem.at[5]
        ),
        pltpu.make_async_copy(c_in, c, load_sem.at[6]),
    ]
    for load in heads + tails + loads:
        load.start()
    others = y_has + x_has + (ring_has + wraps if rings > 1 else ())
    peers = 1 + sum(jnp.where(has, 1, 0) for has in others)
    pl.semaphore_wait(barrier, peers)
    for load in heads:
        load.wait()
    sending(0, 0, lambda copy: copy.start())
    for load in tails:
        load.wait()

    for chunk in range(1, CHUNKS):
        sending(0, chunk, lambda copy: copy.start())
    on_sides(x_has, lambda side: x_start(0, side).start())

    nothing = jnp.zeros((depth, levels), jnp.float32)

    def clear_plane(side):
        @pl.when(jnp.logical_not(y_has[side]))
        def _():
            def one(row, carry):
                for ref in field:
                    ref[(0, planes + 1)[side], row + 1] = nothing
                return carry

            lax.fori_loop(0, rows, one, 0)

    def clear_row(side):
        @pl.when(jnp.logical_not(x_has[side]))
        def _():
            for ref in field:
                for plane in range(planes):
                    ref[plane + 1, (0, rows + 1)[side]] = nothing

    for side in (0, 1):
        clear_plane(side)
        clear_row(side)

    below, above = (lev == 1), (lev == 0)
    place = lax.broadcasted_iota(jnp.int32, (depth, levels), 0)

    def keep_face(t, plane, row, values):
        face = jnp.where(above, values[depth - 1 :], values[:1])
        z_out[t, plane, pl.ds(row, 1)] = face

    def advance(t, plane, row):
        now, other = field[t % 2], field[1 - t % 2]
        last = t == STEPS - 1
        middle = now[plane + 1, row + 1]
        beside = z_in[t, plane, pl.ds(row, 1)]
        lower = jnp.where(place == 0, jnp.where(below, beside, 0.0), pltpu.roll(middle, 1, 0))
        upper = jnp.where(
            place == depth - 1, jnp.where(above, beside, 0.0), pltpu.roll(middle, depth - 1, 0)
        )
        total = now[plane + 1, row] + now[plane + 1, row + 2] + lower + upper
        if not (last and plane == 0):
            total = total + now[plane, row + 1]
        if not (last and plane == planes - 1):
            total = total + now[plane + 2, row + 1]
        spread = total - 6.0 * middle
        later = 2.0 * middle - other[plane + 1, row + 1] + c[plane, row] * spread
        if last:
            out[plane, row] = later
        else:
            other[plane + 1, row + 1] = later
            keep_face(t + 1, plane, row, later)

    for load in loads:
        load.wait()

    def first_face(row, carry):
        for plane in range(planes):
            keep_face(0, plane, row, even[plane + 1, row + 1])
        return carry

    lax.fori_loop(0, rows, first_face, 0)
    z_copy(0).start()
    for way, origin, relay, dest, count in detours:

        @pl.when(lat == relay)
        def _():
            hop(way, relay, count).wait_recv()
            forward(way, dest, count).start()


    for t in range(STEPS):
        last = t == STEPS - 1
        if t > 0:
            on_sides(x_has, lambda side: x_start(t - 1, side).wait_send())
        on_sides(x_has, lambda side: x_arrival(t, side).wait_recv())
        z_copy(t).wait_recv()

        def inside(row, carry):
            for plane in range(planes) if last else range(1, planes - 1):
                advance(t, plane, row)
            return carry

        lax.fori_loop(0, rows, inside, 0)
        if last:
            break

        for chunk in range(CHUNKS):
            if t > 0:
                sending(t - 1, chunk, lambda copy: copy.wait_send())
            for side in (0, 1):
                arriving(t, side, chunk)

            def one(row, carry):
                for plane in (0, planes - 1):
                    advance(t, plane, row)
                return carry

            lax.fori_loop(CUTS[chunk], CUTS[chunk + 1], one, 0)
            sending(t + 1, chunk, lambda copy: copy.start())
            if t + 1 == STEPS - 1 and chunk == CHUNKS - 1:
                for piece in range(CHUNKS, LAST_CHUNKS):
                    sending(t + 1, piece, lambda copy: copy.start())

        on_sides(x_has, lambda side: x_start(t + 1, side).start())
        z_copy(t + 1).start()

    for way, origin, relay, dest, count in detours:
        pl.when(lat == relay)(lambda: forward(way, dest, count).wait_send())
    t = STEPS - 1
    on_sides(x_has, lambda side: x_start(t, side).wait_send())
    for step in range(STEPS):
        z_copy(step).wait_send()

    for chunk in range(CHUNKS):
        sending(t - 1, chunk, lambda copy: copy.wait_send())
    for chunk in range(LAST_CHUNKS):

        def add(side):
            y_arrival(t, side, chunk).wait_recv()
            plane = (0, planes - 1)[side]

            def one(row, carry):
                halo = field[t % 2][(0, planes + 1)[side], row + 1]
                out[plane, row] = out[plane, row] + c[plane, row] * halo
                return carry

            lax.fori_loop(LAST_CUTS[chunk], LAST_CUTS[chunk + 1], one, 0, unroll=4)

        on_sides(y_has, add)
        sending(t, chunk, lambda copy: copy.wait_send())


def shards(pressure, earlier, speed_square):
    planes, rows, depth, levels = pressure.shape
    padded = (planes + 2, rows + 2, depth, levels)
    return pl.pallas_call(
        kernel,
        out_shape=pltpu.VMEM(pressure.shape, jnp.float32),
        in_specs=[pl.BlockSpec(memory_space=pltpu.HBM)] * 3,
        out_specs=pl.BlockSpec(memory_space=pltpu.VMEM),
        scratch_shapes=[
            pltpu.VMEM(padded, jnp.float32),
            pltpu.VMEM(padded, jnp.float32),
            pltpu.VMEM(pressure.shape, jnp.float32),
            pltpu.VMEM((STEPS, planes, rows, levels), jnp.float32),
            pltpu.VMEM((STEPS, planes, rows, levels), jnp.float32),
            pltpu.VMEM((RING * RELIEF,) + pressure.shape[2:], jnp.float32),
            pltpu.SemaphoreType.DMA((7,)),
            pltpu.SemaphoreType.DMA((STEPS, 2, LAST_CHUNKS)),
            pltpu.SemaphoreType.DMA((STEPS, 2, LAST_CHUNKS)),
            pltpu.SemaphoreType.DMA((STEPS, 2)),
            pltpu.SemaphoreType.DMA((STEPS, 2)),
            pltpu.SemaphoreType.DMA((STEPS,)),
            pltpu.SemaphoreType.DMA((STEPS,)),
            pltpu.SemaphoreType.DMA((4,)),
        ],
        compiler_params=pltpu.CompilerParams(
            collective_id=0, has_side_effects=True, vmem_limit_bytes=48 * 2**20
        ),
    )(pressure, earlier, speed_square)


def solution(mesh):
    spec = P("lat", "lon", "lev", None)
    return jax.shard_map(
        shards, mesh=mesh, in_specs=(spec,) * 3, out_specs=spec, check_vma=False
    )
```

```python
import jax
import jax.numpy as jnp
from jax import lax
from jax.experimental import pallas as pl
from jax.experimental.pallas import tpu as pltpu
from jax.sharding import PartitionSpec as P

STEPS = 4
CUTS = (0, 32, 64)
LAST_CUTS = (0, 32, 60, 64)
CHUNKS = len(CUTS) - 1
LAST_CHUNKS = len(LAST_CUTS) - 1
RING = 4
RELIEF = 3
MESH = pl.DeviceIdType.MESH


def kernel(
    p_in, e_in, c_in, out, even, odd, c, z_out, z_in,
    passed, load_sem, y_send, y_recv, x_send, x_recv, z_send, z_recv, hop_sem,
):
    planes, rows, depth, levels = p_in.shape
    lat, lon, lev = (lax.axis_index(name) for name in ("lat", "lon", "lev"))
    field = (even, odd)
    y_has = (lat > 0, lat < lax.axis_size("lat") - 1)
    x_has = (lon > 0, lon < lax.axis_size("lon") - 1)
    y_to = ({"lat": lat - 1}, {"lat": lat + 1})
    x_to = ({"lon": lon - 1}, {"lon": lon + 1})
    z_to = {"lev": 1 - lev}

    rings = lax.axis_size("lat") // RING
    detours = []
    for q in range(rings - 1):
        end, start = q * RING + RING - 1, q * RING + RING
        detours.append((1, end, end + RING, start, RELIEF * (q + 1)))
        detours.append((0, start, start - RING, end, RELIEF * (rings - 1 - q)))
    ring_place = lax.rem(lat, RING)
    at_start, at_end = (ring_place == 0), (ring_place == RING - 1)
    wraps = (at_start, at_end)

    def hop(side, relay, count):
        return pltpu.make_async_remote_copy(
            src_ref=field[0].at[(1, planes)[side], pl.ds(1 + CUTS[2] - count, count)],
            dst_ref=passed.at[pl.ds(0, count)],
            send_sem=hop_sem.at[0],
            recv_sem=hop_sem.at[1],
            device_id={"lat": relay},
            device_id_type=MESH,
        )

    def forward(side, dest, count):
        return pltpu.make_async_remote_copy(
            src_ref=passed.at[pl.ds(0, count)],
            dst_ref=field[0].at[(planes + 1, 0)[side], pl.ds(1 + CUTS[2] - count, count)],
            send_sem=hop_sem.at[2],
            recv_sem=hop_sem.at[3],
            device_id={"lat": dest},
            device_id_type=MESH,
        )

    def y_rows(t, chunk, less=0):
        cuts = LAST_CUTS if t == STEPS - 1 else CUTS
        return pl.ds(1 + cuts[chunk], cuts[chunk + 1] - cuts[chunk] - less)

    def y_start(t, side, chunk, less=0):
        return pltpu.make_async_remote_copy(
            src_ref=field[t % 2].at[(1, planes)[side], y_rows(t, chunk, less)],
            dst_ref=field[t % 2].at[(planes + 1, 0)[side], y_rows(t, chunk, less)],
            send_sem=y_send.at[t, side, chunk],
            recv_sem=y_recv.at[t, 1 - side, chunk],
            device_id=y_to[side],
            device_id_type=MESH,
        )

    def y_arrival(t, side, chunk, less=0):
        halo = field[t % 2].at[(0, planes + 1)[side], y_rows(t, chunk, less)]
        return pltpu.make_async_remote_copy(
            src_ref=halo,
            dst_ref=halo,
            send_sem=y_send.at[t, side, chunk],
            recv_sem=y_recv.at[t, side, chunk],
            device_id=y_to[side],
            device_id_type=MESH,
        )

    def sending(t, chunk, action):
        detoured = t == 0 and chunk == 1
        for side in (1, 0):
            direct = y_has[side]
            if detoured:
                direct = direct & jnp.logical_not(wraps[side])
            pl.when(direct)(lambda side=side: action(y_start(t, side, chunk)))
        for side, origin, relay, dest, count in detours if detoured else ():

            @pl.when(lat == origin)
            def _():
                action(y_start(t, side, chunk, count))
                action(hop(side, relay, count))

    def arriving(t, side, chunk):
        detoured = t == 0 and chunk == 1
        direct = y_has[side]
        if detoured:
            direct = direct & jnp.logical_not(wraps[side])
        pl.when(direct)(lambda: y_arrival(t, side, chunk).wait_recv())
        for way, origin, relay, dest, count in detours if detoured else ():
            if way != side:

                @pl.when(lat == dest)
                def _():
                    y_arrival(t, side, chunk, count).wait_recv()
                    forward(way, dest, count).wait_recv()

    def x_start(t, side):
        if t == 0:
            source = p_in.at[:, (0, rows - 1)[side]]
        else:
            source = field[t % 2].at[pl.ds(1, planes), (1, rows)[side]]
        return pltpu.make_async_remote_copy(
            src_ref=source,
            dst_ref=field[t % 2].at[pl.ds(1, planes), (rows + 1, 0)[side]],
            send_sem=x_send.at[t, side],
            recv_sem=x_recv.at[t, 1 - side],
            device_id=x_to[side],
            device_id_type=MESH,
        )

    def x_arrival(t, side):
        halo = field[t % 2].at[pl.ds(1, planes), (0, rows + 1)[side]]
        return pltpu.make_async_remote_copy(
            src_ref=halo,
            dst_ref=halo,
            send_sem=x_send.at[t, side],
            recv_sem=x_recv.at[t, side],
            device_id=x_to[side],
            device_id_type=MESH,
        )

    def z_copy(t):
        return pltpu.make_async_remote_copy(
            src_ref=z_out.at[t],
            dst_ref=z_in.at[t],
            send_sem=z_send.at[t],
            recv_sem=z_recv.at[t],
            device_id=z_to,
            device_id_type=MESH,
        )

    def on_sides(has, action):
        for side in (0, 1):
            pl.when(has[side])(lambda side=side: action(side))

    barrier = pltpu.get_barrier_semaphore()

    def greet(device):
        pl.semaphore_signal(barrier, inc=1, device_id=device, device_id_type=MESH)

    on_sides(y_has, lambda side: greet(y_to[side]))
    on_sides(x_has, lambda side: greet(x_to[side]))
    greet(z_to)
    outer = at_start | at_end
    ring_has = (outer & (lat >= RING), outer & (lat < (rings - 1) * RING))
    if rings > 1:
        on_sides(ring_has, lambda side: greet({"lat": lat + (-RING, RING)[side]}))
        on_sides(wraps, lambda side: greet({"lat": lat + (RING - 1, 1 - RING)[side]}))

    def load_pressure(number, first, count, start, length):
        return pltpu.make_async_copy(
            p_in.at[pl.ds(first, count), pl.ds(start, length)],
            even.at[pl.ds(first + 1, count), pl.ds(start + 1, length)],
            load_sem.at[number],
        )

    ends = (0, planes - 1)
    heads = [load_pressure(side, ends[side], 1, 0, CUTS[1]) for side in (0, 1)]
    tails = [
        load_pressure(2 + side, ends[side], 1, CUTS[1], rows - CUTS[1]) for side in (0, 1)
    ]
    loads = [
        load_pressure(4, 1, planes - 2, 0, rows),
        pltpu.make_async_copy(
            e_in, odd.at[pl.ds(1, planes), pl.ds(1, rows)], load_sem.at[5]
        ),
        pltpu.make_async_copy(c_in, c, load_sem.at[6]),
    ]
    for load in heads + tails + loads:
        load.start()
    others = y_has + x_has + (ring_has + wraps if rings > 1 else ())
    peers = 1 + sum(jnp.where(has, 1, 0) for has in others)
    pl.semaphore_wait(barrier, peers)
    for load in heads:
        load.wait()
    sending(0, 0, lambda copy: copy.start())
    for load in tails:
        load.wait()

    for chunk in range(1, CHUNKS):
        sending(0, chunk, lambda copy: copy.start())
    on_sides(x_has, lambda side: x_start(0, side).start())

    nothing = jnp.zeros((depth, levels), jnp.float32)

    def clear_plane(side):
        @pl.when(jnp.logical_not(y_has[side]))
        def _():
            def one(row, carry):
                for ref in field:
                    ref[(0, planes + 1)[side], row + 1] = nothing
                return carry

            lax.fori_loop(0, rows, one, 0)

    def clear_row(side):
        @pl.when(jnp.logical_not(x_has[side]))
        def _():
            for ref in field:
                for plane in range(planes):
                    ref[plane + 1, (0, rows + 1)[side]] = nothing

    for side in (0, 1):
        clear_plane(side)
        clear_row(side)

    below, above = (lev == 1), (lev == 0)
    place = lax.broadcasted_iota(jnp.int32, (depth, levels), 0)

    def keep_face(t, plane, row, values):
        face = jnp.where(above, values[depth - 1 :], values[:1])
        z_out[t, plane, pl.ds(row, 1)] = face

    def advance(t, plane, row):
        now, other = field[t % 2], field[1 - t % 2]
        last = t == STEPS - 1
        middle = now[plane + 1, row + 1]
        beside = z_in[t, plane, pl.ds(row, 1)]
        lower = jnp.where(place == 0, jnp.where(below, beside, 0.0), pltpu.roll(middle, 1, 0))
        upper = jnp.where(
            place == depth - 1, jnp.where(above, beside, 0.0), pltpu.roll(middle, depth - 1, 0)
        )
        total = now[plane + 1, row] + now[plane + 1, row + 2] + lower + upper
        if not (last and plane == 0):
            total = total + now[plane, row + 1]
        if not (last and plane == planes - 1):
            total = total + now[plane + 2, row + 1]
        spread = total - 6.0 * middle
        later = 2.0 * middle - other[plane + 1, row + 1] + c[plane, row] * spread
        if last:
            out[plane, row] = later
        else:
            other[plane + 1, row + 1] = later
            keep_face(t + 1, plane, row, later)

    for load in loads:
        load.wait()

    def first_face(row, carry):
        for plane in range(planes):
            keep_face(0, plane, row, even[plane + 1, row + 1])
        return carry

    lax.fori_loop(0, rows, first_face, 0)
    z_copy(0).start()
    for way, origin, relay, dest, count in detours:

        @pl.when(lat == relay)
        def _():
            hop(way, relay, count).wait_recv()
            forward(way, dest, count).start()


    for t in range(STEPS):
        last = t == STEPS - 1
        if t > 0:
            on_sides(x_has, lambda side: x_start(t - 1, side).wait_send())
        on_sides(x_has, lambda side: x_arrival(t, side).wait_recv())
        z_copy(t).wait_recv()

        def inside(row, carry):
            for plane in range(planes) if last else range(1, planes - 1):
                advance(t, plane, row)
            return carry

        lax.fori_loop(0, rows, inside, 0)
        if last:
            break

        for chunk in range(CHUNKS):
            if t > 0:
                sending(t - 1, chunk, lambda copy: copy.wait_send())
            for side in (0, 1):
                arriving(t, side, chunk)

            def one(row, carry):
                for plane in (0, planes - 1):
                    advance(t, plane, row)
                return carry

            lax.fori_loop(CUTS[chunk], CUTS[chunk + 1], one, 0)
            sending(t + 1, chunk, lambda copy: copy.start())
            if t + 1 == STEPS - 1 and chunk == CHUNKS - 1:
                for piece in range(CHUNKS, LAST_CHUNKS):
                    sending(t + 1, piece, lambda copy: copy.start())

        on_sides(x_has, lambda side: x_start(t + 1, side).start())
        z_copy(t + 1).start()

    for way, origin, relay, dest, count in detours:
        pl.when(lat == relay)(lambda: forward(way, dest, count).wait_send())
    t = STEPS - 1
    on_sides(x_has, lambda side: x_start(t, side).wait_send())
    for step in range(STEPS):
        z_copy(step).wait_send()

    for chunk in range(CHUNKS):
        sending(t - 1, chunk, lambda copy: copy.wait_send())
    for chunk in range(LAST_CHUNKS):

        def add(side):
            y_arrival(t, side, chunk).wait_recv()
            plane = (0, planes - 1)[side]

            def one(row, carry):
                halo = field[t % 2][(0, planes + 1)[side], row + 1]
                out[plane, row] = out[plane, row] + c[plane, row] * halo
                return carry

            lax.fori_loop(LAST_CUTS[chunk], LAST_CUTS[chunk + 1], one, 0, unroll=4)

        sending(t, chunk, lambda copy: copy.wait_send())
        on_sides(y_has, add)


def shards(pressure, earlier, speed_square):
    planes, rows, depth, levels = pressure.shape
    padded = (planes + 2, rows + 2, depth, levels)
    return pl.pallas_call(
        kernel,
        out_shape=pltpu.VMEM(pressure.shape, jnp.float32),
        in_specs=[pl.BlockSpec(memory_space=pltpu.HBM)] * 3,
        out_specs=pl.BlockSpec(memory_space=pltpu.VMEM),
        scratch_shapes=[
            pltpu.VMEM(padded, jnp.float32),
            pltpu.VMEM(padded, jnp.float32),
            pltpu.VMEM(pressure.shape, jnp.float32),
            pltpu.VMEM((STEPS, planes, rows, levels), jnp.float32),
            pltpu.VMEM((STEPS, planes, rows, levels), jnp.float32),
            pltpu.VMEM((RING * RELIEF,) + pressure.shape[2:], jnp.float32),
            pltpu.SemaphoreType.DMA((7,)),
            pltpu.SemaphoreType.DMA((STEPS, 2, LAST_CHUNKS)),
            pltpu.SemaphoreType.DMA((STEPS, 2, LAST_CHUNKS)),
            pltpu.SemaphoreType.DMA((STEPS, 2)),
            pltpu.SemaphoreType.DMA((STEPS, 2)),
            pltpu.SemaphoreType.DMA((STEPS,)),
            pltpu.SemaphoreType.DMA((STEPS,)),
            pltpu.SemaphoreType.DMA((4,)),
        ],
        compiler_params=pltpu.CompilerParams(
            collective_id=0, has_side_effects=True, vmem_limit_bytes=48 * 2**20
        ),
    )(pressure, earlier, speed_square)


def solution(mesh):
    spec = P("lat", "lon", "lev", None)
    return jax.shard_map(
        shards, mesh=mesh, in_specs=(spec,) * 3, out_specs=spec, check_vma=False
    )
```
